32 devices in a mesh: pod: 2 (over x), dp: 4 (over z), sp: 4 (over y, core).
Axes of the slice: x: 2, y: 2, z: 4, core: 2. Of those that a mesh axis runs over, the one named last changes fastest.
Arguments:
- images: bfloat16 [24, 512, 64, 64], P(('pod', 'dp'), 'sp'), parts along dimension 0
- w_a: bfloat16 [1, 3, 3, 64, 64], replicated
- norm_a: float32 [1, 2, 64], replicated
- w_down: bfloat16 [3, 3, 64, 128], replicated
- norm_down: float32 [2, 128], replicated
- w_b: bfloat16 [3, 3, 3, 128, 128], replicated
- norm_b: float32 [3, 2, 128], replicated
Outputs:
- output: bfloat16 [24, 256, 32, 128], P(('pod', 'dp'), 'sp'), parts along dimension 0
There are 2 independent parts. The reference program is written for one: setup_inputs(seed, part) draws one part's arguments, and reference() takes and returns one part's arrays. A program takes and returns all parts, laid end to end along the dimension named above; an argument that names none is the same for every part.
All inputs are finite; a program needn't handle non-finite values.
Results may differ from the reference program's by a relative error of at most 0.00451443.
Values are sent between devices in bfloat16 or wider.
A program may use at most 1 GiB of HBM per device.

```python
import jax
import jax.numpy as jnp
from jax import lax

BATCH = 12
HEIGHT = 512
WIDTH = 64
CH_A = 64
CH_B = 128
LAYERS_A = 1
LAYERS_B = 3
EPS_VALUE = 1e-5
CONV_DIMS = ('NHWC', 'HWIO', 'NHWC')


def setup_inputs(seed: int = 0, part: int = 0) -> dict:
    base_key = jax.random.key(seed)
    part_key = jax.random.fold_in(base_key, part)
    noise_key, dir_key, scale_key, offset_key, phase_key = jax.random.split(part_key, 5)
    weight_keys = jax.random.split(base_key, 9)
    row_pos = jnp.arange(HEIGHT, dtype=jnp.float32) * (2.0 / (HEIGHT - 1)) - 1.0
    row_col = row_pos[None, :, None, None]
    noise = jax.random.normal(noise_key, (BATCH, HEIGHT, WIDTH, CH_A), jnp.float32)
    chan_dir = jax.random.normal(dir_key, (BATCH, 1, 1, CH_A), jnp.float32)
    img_scale = jax.random.uniform(scale_key, (BATCH, 1, 1, 1), jnp.float32, 0.5, 1.5)
    img_offset = 0.5 * jax.random.normal(offset_key, (BATCH, 1, 1, CH_A), jnp.float32)
    phase = jax.random.uniform(phase_key, (BATCH, 1, 1, CH_A), jnp.float32, 0.0, 6.2831853)
    wave = 0.5 * jnp.sin(row_col * 7.0 + phase)
    x_val = img_scale * (0.7 * noise + row_col * chan_dir + wave) + img_offset
    w_a = jax.random.normal(weight_keys[0], (LAYERS_A, 3, 3, CH_A, CH_A), jnp.float32) * (9 * CH_A) ** -0.5
    norm_a = jnp.stack([jax.random.uniform(weight_keys[1], (LAYERS_A, CH_A), jnp.float32, 0.6, 1.4), 0.3 * jax.random.normal(weight_keys[2], (LAYERS_A, CH_A), jnp.float32)], axis=1)
    w_down = jax.random.normal(weight_keys[3], (3, 3, CH_A, CH_B), jnp.float32) * (9 * CH_A) ** -0.5
    norm_down = jnp.stack([jax.random.uniform(weight_keys[4], (CH_B,), jnp.float32, 0.6, 1.4), 0.3 * jax.random.normal(weight_keys[5], (CH_B,), jnp.float32)])
    w_b = jax.random.normal(weight_keys[6], (LAYERS_B, 3, 3, CH_B, CH_B), jnp.float32) * (9 * CH_B) ** -0.5
    norm_b = jnp.stack([jax.random.uniform(weight_keys[7], (LAYERS_B, CH_B), jnp.float32, 0.6, 1.4), 0.3 * jax.random.normal(weight_keys[8], (LAYERS_B, CH_B), jnp.float32)], axis=1)
    return {'images': x_val.astype(jnp.bfloat16), 'w_a': w_a.astype(jnp.bfloat16), 'norm_a': norm_a, 'w_down': w_down.astype(jnp.bfloat16), 'norm_down': norm_down, 'w_b': w_b.astype(jnp.bfloat16), 'norm_b': norm_b}


def conv_norm(hidden, weight, norm_pair, stride, pads):
    z_val = lax.conv_general_dilated(hidden.astype(jnp.float32), weight.astype(jnp.float32), (stride, stride), pads, dimension_numbers=CONV_DIMS)
    mean_val = jnp.mean(z_val, axis=(0, 1, 2))
    mean_sq = jnp.mean(z_val * z_val, axis=(0, 1, 2))
    inv_std = lax.rsqrt(mean_sq - mean_val * mean_val + EPS_VALUE)
    scaled = norm_pair[0] * (z_val - mean_val) * inv_std + norm_pair[1]
    return jnp.maximum(scaled, 0.0).astype(jnp.bfloat16)


def reference(images, w_a, norm_a, w_down, norm_down, w_b, norm_b):
    def same_step(hidden, layer_args):
        return conv_norm(hidden, layer_args[0], layer_args[1], 1, ((1, 1), (1, 1))), None
    hidden, unused_a = lax.scan(same_step, images, (w_a, norm_a))
    hidden = conv_norm(hidden, w_down, norm_down, 2, ((0, 1), (0, 1)))
    hidden, unused_b = lax.scan(same_step, hidden, (w_b, norm_b))
    return hidden
```

```python
import functools

import jax
import jax.numpy as jnp
from jax import lax
from jax.experimental import pallas as pl
from jax.experimental.pallas import tpu as pltpu
from jax.sharding import PartitionSpec as P

EPS_VALUE = 1e-5
F32 = jnp.float32
BF16 = jnp.bfloat16
NB = 3
MESH = pl.DeviceIdType.MESH


def fused_kernel(dp_size, sp_size, img, wa, na, wd, nd, wb, nb, out,
                 xv, t32, pa, za, sa, sh, zb, yb, wam, wdm, wbm,
                 wav, nav, wdv, ndv, wbv, nbv, st, o32, ov,
                 img_sem, w_sem, st_send, st_recv, halo_send, halo_recv, out_sem):
    group = dp_size * sp_size
    pod = lax.axis_index("pod")
    dp = lax.axis_index("dp")
    sp = lax.axis_index("sp")
    me = dp * sp_size + sp
    is_top = sp == 0
    is_bottom = sp == sp_size - 1

    def peer_id(k):
        peer = lax.rem(me + k, group)
        return (pod, lax.div(peer, sp_size), lax.rem(peer, sp_size))

    barrier = pltpu.get_barrier_semaphore()
    for k in range(1, group):
        pl.semaphore_signal(barrier, inc=1, device_id=peer_id(k), device_id_type=MESH)

    img_copies = [pltpu.make_async_copy(img.at[n], xv.at[n, pl.ds(64, 4096)], img_sem.at[n]) for n in range(NB)]
    for copy in img_copies:
        copy.start()
    w_copies = [pltpu.make_async_copy(src, dst, w_sem.at[i]) for i, (src, dst) in enumerate(
        [(wa, wav), (na, nav), (wd, wdv), (nd, ndv), (wb, wbv), (nb, nbv)])]
    for copy in w_copies:
        copy.start()

    for n in range(NB):
        xv[n, 0:64] = jnp.zeros((64, 128), BF16)
        xv[n, 4160:4224] = jnp.zeros((64, 128), BF16)
        sa[0, n, 16, 0] = jnp.zeros((64, 128), BF16)
        sh[n, 16, 0] = jnp.zeros((64, 128), BF16)
        for p in range(3):
            yb[p, n, 0, 0] = jnp.zeros((64, 128), BF16)
            yb[p, n, 16, 1] = jnp.zeros((64, 128), BF16)

    @pl.when(is_top)
    def _():
        t32[:, :, 7:8, :] = jnp.zeros((NB, 33, 1, 128), F32)
        zb[:, :, :, :, 7:8, :] = jnp.zeros((2, 2, NB, 16, 1, 128), F32)

    @pl.when(is_bottom)
    def _():
        t32[:, :, 136:137, :] = jnp.zeros((NB, 33, 1, 128), F32)
        za[:, :, :, 64:65, :] = jnp.zeros((2, NB, 32, 1, 128), F32)
        zb[:, :, :, :, 72:73, :] = jnp.zeros((2, 2, NB, 16, 1, 128), F32)

    for copy in w_copies:
        copy.wait()

    zero64 = jnp.zeros((64, 64), BF16)
    for t in range(4):
        for u in range(4):
            parts = []
            for cp in range(2):
                for rp in range(2):
                    p, q = t - rp, u - cp
                    ok = 0 <= p <= 2 and 0 <= q <= 2
                    parts.append(wav[0, p, q] if ok else zero64)
            row = t * 256 + u * 64
            wam[row:row + 64, :] = jnp.concatenate(parts, axis=1)

    def down_tap(v, p):
        cols = []
        for jp in range(2):
            q = v - 2 * jp
            cols.append(wdv[p, q] if 0 <= q <= 2 else jnp.zeros((64, 128), BF16))
        return jnp.concatenate(cols, axis=1)

    for v in range(5):
        for rp in range(2):
            wdm[v * 128 + rp * 64:v * 128 + rp * 64 + 64, :] = down_tap(v, rp)
    for v in range(6):
        wdm[640 + v * 64:640 + v * 64 + 64, :] = down_tap(v, 2)

    for layer in range(3):
        for p in range(3):
            for u in range(4):
                for jp in range(2):
                    q = u - jp
                    blk = wbv[layer, p, q] if 0 <= q <= 2 else jnp.zeros((128, 128), BF16)
                    row = (p * 4 + u) * 128
                    wbm[layer, row:row + 128, jp * 128:jp * 128 + 128] = blk

    for n in range(NB):
        img_copies[n].wait()

        def to_rows(a, carry, n=n):
            tile = xv[n, pl.ds(pl.multiple_of(a * 128, 128), 128), :]
            t32[n, a, 8:136, :] = tile.T.astype(F32)
            return carry
        lax.fori_loop(0, 33, to_rows, 0)

    pl.semaphore_wait(barrier, group - 1)

    def exchange(idx, top_src, bottom_src, top_dst, bottom_dst):
        up = pltpu.make_async_remote_copy(top_src, bottom_dst, halo_send.at[idx, 0], halo_recv.at[idx, 0],
                                          device_id=(pod, dp, lax.rem(sp + sp_size - 1, sp_size)), device_id_type=MESH)
        down = None
        if bottom_src is not None:
            down = pltpu.make_async_remote_copy(bottom_src, top_dst, halo_send.at[idx, 1], halo_recv.at[idx, 1],
                                                device_id=(pod, dp, lax.rem(sp + 1, sp_size)), device_id_type=MESH)

        def start():
            @pl.when(sp > 0)
            def _():
                up.start()
            if down is not None:
                @pl.when(sp < sp_size - 1)
                def _():
                    down.start()

        def wait():
            @pl.when(sp > 0)
            def _():
                up.wait_send()
                if down is not None:
                    down.wait_recv()

            @pl.when(sp < sp_size - 1)
            def _():
                up.wait_recv()
                if down is not None:
                    down.wait_send()
        return start, wait

    start, wait = exchange(0, t32.at[:, :, pl.ds(8, 1), :], t32.at[:, :, pl.ds(135, 1), :],
                           t32.at[:, :, pl.ds(7, 1), :], t32.at[:, :, pl.ds(136, 1), :])
    start()

    def split_rows(taps):
        def body(a, carry):
            for n in range(NB):
                for t in taps:
                    pa[t, n, a] = t32[n, a, pl.ds(7 + t, 64, stride=2), :].astype(BF16)
            return carry
        lax.fori_loop(0, 33, body, 0)

    split_rows((1, 2))
    wait()
    split_rows((0, 3))

    def sums(z_val, carry):
        s1, s2 = carry
        z8 = z_val.reshape(64, 8, 256)
        return s1 + jnp.sum(z8, axis=0), s2 + jnp.sum(z8 * z8, axis=0)

    zero_sums = (jnp.zeros((8, 256), F32), jnp.zeros((8, 256), F32))

    def send_sums(layer, carry):
        rows = []
        for s in carry:
            r = jnp.sum(s, axis=0, keepdims=True)
            rows.append(r[:, :128] + r[:, 128:])
        st[layer, me] = jnp.concatenate(rows, axis=0)
        for k in range(1, group):
            pltpu.make_async_remote_copy(st.at[layer, me], st.at[layer, me], st_send.at[layer], st_recv.at[layer],
                                         device_id=peer_id(k), device_id_type=MESH).start()

    def recv_sums(layer, gamma, beta, count, fold):
        others = st.at[layer, pl.ds(0, group - 1)]
        pltpu.make_async_copy(others, others, st_recv.at[layer]).wait()
        pltpu.make_async_copy(others, others, st_send.at[layer]).wait()
        total = jnp.sum(st[layer], axis=0)
        if fold:
            total = total + pltpu.roll(total, 64, 1)
        mean = total[0:1] / count
        var = total[1:2] / count - mean * mean
        scale = gamma * lax.rsqrt(var + EPS_VALUE)
        return scale, beta - mean * scale

    def conv_a(it, carry):
        n = lax.div(it, 4)
        a0 = lax.rem(it, 4) * 8
        parts = []
        for t in range(4):
            parts.append(pa[t, n, pl.ds(a0, 8)].reshape(512, 128))
            parts.append(pa[t, n, pl.ds(a0 + 1, 8)].reshape(512, 128))
        z_val = jnp.dot(jnp.concatenate(parts, axis=1), wam[...], preferred_element_type=F32)
        for cp in range(2):
            za[cp, n, pl.ds(a0, 8), 0:64, :] = z_val[:, cp * 128:cp * 128 + 128].reshape(8, 64, 128)
        return sums(z_val, carry)

    carry = lax.fori_loop(0, NB * 4, conv_a, zero_sums)
    send_sums(0, carry)
    start, wait = exchange(1, za.at[:, :, :, pl.ds(0, 1), :], None, None, za.at[:, :, :, pl.ds(64, 1), :])
    start()
    pixels = float(NB * 128 * 64 * group)
    gamma = jnp.concatenate([nav[0, 0:1, :]] * 2, axis=1)
    beta = jnp.concatenate([nav[0, 1:2, :]] * 2, axis=1)
    scale, shift = recv_sums(0, gamma, beta, pixels, True)
    wait()

    row_idx = lax.broadcasted_iota(jnp.int32, (64, 128), 0)
    lane_idx = lax.broadcasted_iota(jnp.int32, (64, 128), 1)
    low_lanes = lane_idx < 64
    cut_top = jnp.logical_and(row_idx == 0, is_top)
    cut_bottom = jnp.logical_and(row_idx == 63, is_bottom)

    def norm_a(it, carry):
        n = lax.div(it, 16)
        g = lax.rem(it, 16)
        for b in range(2):
            a = g * 2 + b
            for cp in range(2):
                y = jnp.maximum(za[cp, n, a, 0:64, :] * scale + shift, 0.0)
                sa[cp, n, g, b] = y.astype(BF16)
            z_next = jnp.where(low_lanes, za[0, n, a, 1:65, :], pltpu.roll(za[1, n, a, 1:65, :], 64, 1))
            y = jnp.maximum(z_next * scale + shift, 0.0)
            sh[n, g, b] = jnp.where(cut_bottom, 0.0, y).astype(BF16)
        return carry
    lax.fori_loop(0, NB * 16, norm_a, 0)

    def store_z(par, n, g0, z_val):
        for jp in range(2):
            zb[par, jp, n, pl.ds(g0, 8), 8:72, :] = z_val[:, jp * 128:jp * 128 + 128].reshape(8, 64, 128)

    def conv_down(it, carry):
        n = lax.div(it, 2)
        g0 = lax.rem(it, 2) * 8
        here, next_ = pl.ds(g0, 8), pl.ds(g0 + 1, 8)
        parts = [sa[0, n, here, 0], sa[1, n, here, 0], sa[0, n, here, 1], sa[1, n, here, 1], sa[0, n, next_, 0],
                 sh[n, here, 0], sh[n, here, 1], sh[n, next_, 0]]
        lhs = jnp.concatenate([x.reshape(512, 128) for x in parts], axis=1)
        z_val = jnp.dot(lhs, wdm[...], preferred_element_type=F32)
        store_z(0, n, g0, z_val)
        return sums(z_val, carry)

    def finish(layer, par, carry, gamma, beta, count, halo):
        send_sums(layer, carry)
        if halo:
            start, wait = exchange(layer + 1, zb.at[par, :, :, :, pl.ds(8, 1), :], zb.at[par, :, :, :, pl.ds(71, 1), :],
                                   zb.at[par, :, :, :, pl.ds(7, 1), :], zb.at[par, :, :, :, pl.ds(72, 1), :])
            start()
        scale, shift = recv_sums(layer, gamma, beta, count, False)
        if halo:
            wait()
        return scale, shift

    carry = lax.fori_loop(0, NB * 2, conv_down, zero_sums)
    pixels = float(NB * 64 * 32 * group)
    scale, shift = finish(1, 0, carry, ndv[0:1], ndv[1:2], pixels, True)

    for layer in range(3):
        par = layer % 2

        def norm_b(it, carry, par=par, scale=scale, shift=shift):
            n = lax.div(it, 16)
            g = lax.rem(it, 16)
            for jp in range(2):
                for p in range(3):
                    y = jnp.maximum(zb[par, jp, n, g, 7 + p:71 + p, :] * scale + shift, 0.0)
                    if p == 0:
                        y = jnp.where(cut_top, 0.0, y)
                    if p == 2:
                        y = jnp.where(cut_bottom, 0.0, y)
                    yb[p, n, g + jp, 1 - jp] = y.astype(BF16)
            return carry
        lax.fori_loop(0, NB * 16, norm_b, 0)

        def conv_b(it, carry, layer=layer, par=par):
            n = lax.div(it, 2)
            g0 = lax.rem(it, 2) * 8
            parts = []
            for p in range(3):
                for u in range(4):
                    parts.append(yb[p, n, pl.ds(g0 + u // 2, 8), u % 2].reshape(512, 128))
            z_val = jnp.dot(jnp.concatenate(parts, axis=1), wbm[layer], preferred_element_type=F32)
            store_z(1 - par, n, g0, z_val)
            return sums(z_val, carry)
        carry = lax.fori_loop(0, NB * 2, conv_b, zero_sums)
        scale, shift = finish(layer + 2, 1 - par, carry, nbv[layer, 0:1], nbv[layer, 1:2], pixels, layer < 2)

    out_copies = []
    for n in range(NB):
        def norm_out(g, carry, n=n):
            for jp in range(2):
                y = jnp.maximum(zb[1, jp, n, g, 8:72, :] * scale + shift, 0.0)
                o32[n, pl.ds(g * 2 + jp, 64, stride=33), :] = y
            return carry
        lax.fori_loop(0, 16, norm_out, 0)

        def pack_out(i, carry, n=n):
            ov[n, i] = o32[n, pl.ds(i * 33, 32), :].astype(BF16)
            return carry
        lax.fori_loop(0, 64, pack_out, 0)
        copy = pltpu.make_async_copy(ov.at[n], out.at[n], out_sem.at[n])
        copy.start()
        out_copies.append(copy)
    for copy in out_copies:
        copy.wait()


def solution(mesh):
    dp_size, sp_size = mesh.shape["dp"], mesh.shape["sp"]
    group = dp_size * sp_size

    def body(images, w_a, norm_a, w_down, norm_down, w_b, norm_b):
        img = jnp.transpose(images, (0, 2, 3, 1)).reshape(NB, 4096, 128)
        vm = pltpu.VMEM
        any_spec = pl.BlockSpec(memory_space=pl.ANY)
        return pl.pallas_call(
            functools.partial(fused_kernel, dp_size, sp_size),
            out_shape=jax.ShapeDtypeStruct((NB, 64, 32, 128), BF16),
            in_specs=[any_spec] * 7,
            out_specs=any_spec,
            scratch_shapes=[
                vm((NB, 4224, 128), BF16),
                vm((NB, 33, 144, 128), F32),
                vm((4, NB, 33, 64, 128), BF16),
                vm((2, NB, 32, 72, 128), F32),
                vm((2, NB, 17, 2, 64, 128), BF16),
                vm((NB, 17, 2, 64, 128), BF16),
                vm((2, 2, NB, 16, 80, 128), F32),
                vm((3, NB, 17, 2, 64, 128), BF16),
                vm((1024, 256), BF16),
                vm((1024, 256), BF16),
                vm((3, 1536, 256), BF16),
                vm((1, 3, 3, 64, 64), BF16),
                vm((1, 2, 64), F32),
                vm((3, 3, 64, 128), BF16),
                vm((2, 128), F32),
                vm((3, 3, 3, 128, 128), BF16),
                vm((3, 2, 128), F32),
                vm((5, group, 2, 128), F32),
                vm((NB, 64 * 33, 128), F32),
                vm((NB, 64, 32, 128), BF16),
                pltpu.SemaphoreType.DMA((NB,)),
                pltpu.SemaphoreType.DMA((6,)),
                pltpu.SemaphoreType.DMA((5,)),
                pltpu.SemaphoreType.DMA((5,)),
                pltpu.SemaphoreType.DMA((5, 2)),
                pltpu.SemaphoreType.DMA((5, 2)),
                pltpu.SemaphoreType.DMA((NB,)),
            ],
            compiler_params=pltpu.CompilerParams(
                collective_id=0, has_side_effects=True, vmem_limit_bytes=62 * 1024 * 1024),
        )(img, w_a, norm_a, w_down, norm_down, w_b, norm_b)

    act_spec = P(("pod", "dp"), "sp", None, None)
    return jax.shard_map(body, mesh=mesh, in_specs=(act_spec, P(), P(), P(), P(), P(), P()), out_specs=act_spec, check_vma=False)
```

```python
import functools

import jax
import jax.numpy as jnp
from jax import lax
from jax.experimental import pallas as pl
from jax.experimental.pallas import tpu as pltpu
from jax.sharding import PartitionSpec as P

EPS_VALUE = 1e-5
F32 = jnp.float32
BF16 = jnp.bfloat16
NB = 3
MESH = pl.DeviceIdType.MESH


def fused_kernel(dp_size, sp_size, img, wa, na, wd, nd, wb, nb, out,
                 xv, t32, pa0, pa1, za, sa0, sa1, zb, yb0, yb1, wam, wdm, wbm,
                 wav, nav, wdv, ndv, wbv, nbv, st, o32, hs, hr,
                 img_sem, w_sem, st_send, st_recv, halo_send, halo_recv):
    group = dp_size * sp_size
    pod = lax.axis_index("pod")
    dp = lax.axis_index("dp")
    sp = lax.axis_index("sp")
    me = dp * sp_size + sp
    is_top = sp == 0
    is_bottom = sp == sp_size - 1

    dp_order = [dp_size - 1 - dp, lax.rem(dp + 2, dp_size), dp + 1 - 2 * lax.rem(dp, 2), dp]
    sp_order = [lax.rem(sp + off, sp_size) for off in (2, 1, 3, 0)]
    peers = [(pod, d, s) for d in dp_order for s in sp_order][:group - 1]

    barrier = pltpu.get_barrier_semaphore()
    for peer in peers:
        pl.semaphore_signal(barrier, inc=1, device_id=peer, device_id_type=MESH)

    img_copies = [pltpu.make_async_copy(img.at[n], xv.at[n, pl.ds(64, 4096)], img_sem.at[n]) for n in range(NB)]
    w_copies = [pltpu.make_async_copy(src, dst, w_sem.at[i]) for i, (src, dst) in enumerate(
        [(wa, wav), (na, nav), (wd, wdv), (nd, ndv), (wb, wbv), (nb, nbv)])]
    for copy in (w_copies[0], *img_copies, *w_copies[1:]):
        copy.start()

    zero_tile = jnp.zeros((64, 128), BF16)
    zero_row = jnp.zeros((NB, 33, 1, 128), F32)
    for n in range(NB):
        xv[n, 0:64] = zero_tile
        xv[n, 4160:4224] = zero_tile
    t32[:, :, 7:8, :] = zero_row
    t32[:, :, 136:137, :] = zero_row

    w_copies[0].wait()
    zero64 = jnp.zeros((64, 64), BF16)
    for t in range(4):
        for u in range(4):
            parts = []
            for cp in range(2):
                for rp in range(2):
                    p, q = t - rp, u - cp
                    parts.append(wav[0, p, q] if 0 <= p <= 2 and 0 <= q <= 2 else zero64)
            row = t * 256 + u * 64
            wam[row:row + 64, :] = jnp.concatenate(parts, axis=1)

    for n in range(NB):
        img_copies[n].wait()

        def to_rows(i, carry, n=n):
            for j in range(11):
                a = i * 11 + j
                tile = xv[n, pl.ds(pl.multiple_of(a * 128, 128), 128), :]
                t32[n, a, 8:136, :] = tile.T.astype(F32)
            return carry
        lax.fori_loop(0, 3, to_rows, 0)

    def exchange(idx, has_down):
        up = pltpu.make_async_remote_copy(hs.at[idx, 0], hr.at[idx, 1], halo_send.at[idx, 0], halo_recv.at[idx, 0],
                                          device_id=(pod, dp, lax.rem(sp + sp_size - 1, sp_size)), device_id_type=MESH)
        down = None
        if has_down:
            down = pltpu.make_async_remote_copy(hs.at[idx, 1], hr.at[idx, 0], halo_send.at[idx, 1], halo_recv.at[idx, 1],
                                                device_id=(pod, dp, lax.rem(sp + 1, sp_size)), device_id_type=MESH)

        def start():
            @pl.when(sp > 0)
            def _():
                up.start()
            if has_down:
                @pl.when(sp < sp_size - 1)
                def _():
                    down.start()

        def wait():
            @pl.when(sp > 0)
            def _():
                up.wait_send()
                if has_down:
                    down.wait_recv()

            @pl.when(sp < sp_size - 1)
            def _():
                up.wait_recv()
                if has_down:
                    down.wait_send()
        return start, wait

    t_rows = t32.reshape(NB, 33 * 144, 128)
    for n in range(NB):
        hs[0, 0, n, 0:33, :] = t_rows[n, pl.ds(8, 33, stride=144), :]
        hs[0, 1, n, 0:33, :] = t_rows[n, pl.ds(135, 33, stride=144), :]
    pl.semaphore_wait(barrier, group - 1)
    start, wait_image = exchange(0, True)
    start()

    def split_rows(n, a0, dst):
        for j in range(9):
            for t in range(4):
                dst[t, j] = t32[n, a0 + j, pl.ds(7 + t, 64, stride=2), :].astype(BF16)

    def sums(z_val, carry):
        s1, s2 = carry
        z8 = z_val.reshape(-1, 8, 256)
        return s1 + jnp.sum(z8, axis=0), s2 + jnp.sum(z8 * z8, axis=0)

    zero_sums = (jnp.zeros((8, 256), F32), jnp.zeros((8, 256), F32))

    def send_sums(layer, carry):
        rows = []
        for s in carry:
            r = jnp.sum(s, axis=0, keepdims=True)
            rows.append(r[:, :128] + r[:, 128:])
        st[layer, me] = jnp.concatenate(rows, axis=0)
        for peer in peers:
            pltpu.make_async_remote_copy(st.at[layer, me], st.at[layer, me], st_send.at[layer], st_recv.at[layer],
                                         device_id=peer, device_id_type=MESH).start()

    def recv_sums(layer, gamma, beta, count, fold):
        others = st.at[layer, pl.ds(0, group - 1)]
        pltpu.make_async_copy(others, others, st_recv.at[layer]).wait()
        pltpu.make_async_copy(others, others, st_send.at[layer]).wait()
        total = jnp.sum(st[layer], axis=0)
        if fold:
            total = total + pltpu.roll(total, 64, 1)
        mean = total[0:1] / count
        var = total[1:2] / count - mean * mean
        scale = gamma * lax.rsqrt(var + EPS_VALUE)
        return scale, beta - mean * scale

    def conv_a(n, a0, src, carry):
        parts = []
        for t in range(4):
            parts.append(src[t, 0:8].reshape(512, 128))
            parts.append(src[t, 1:9].reshape(512, 128))
        z_val = jnp.dot(jnp.concatenate(parts, axis=1), wam[...], preferred_element_type=F32)
        for cp in range(2):
            za[cp, n, pl.ds(a0, 8), 0:64, :] = z_val[:, cp * 128:cp * 128 + 128].reshape(8, 64, 128)
        return sums(z_val, carry)

    split_rows(0, 0, pa0)

    def loop_a(i, carry):
        n, a0 = lax.div(i, 2), lax.rem(i, 2) * 16
        after = lax.rem(i + 1, 2 * NB)
        carry = conv_a(n, a0, pa0, carry)
        split_rows(n, a0 + 8, pa1)
        carry = conv_a(n, a0 + 8, pa1, carry)
        split_rows(lax.div(after, 2), lax.rem(after, 2) * 16, pa0)
        return carry

    carry = lax.fori_loop(0, 2 * NB, loop_a, zero_sums)

    wait_image()

    @pl.when(is_top)
    def _():
        hr[0, 0] = jnp.zeros(hr.shape[2:], F32)

    @pl.when(is_bottom)
    def _():
        hr[0, 1] = jnp.zeros(hr.shape[2:], F32)

    s1, s2 = carry
    z_rows = za.reshape(2, NB, 32 * 72, 128)
    for n in range(NB):
        for side, row, w_row in ((0, 0, 0), (1, 63, 768)):
            lhs = jnp.concatenate([hr[0, side, n, 0:32, :], hr[0, side, n, 1:33, :]], axis=1).astype(BF16)
            add = jnp.dot(lhs, wam[w_row:w_row + 256, :], preferred_element_type=F32)
            old = jnp.concatenate([z_rows[cp, n, pl.ds(row, 32, stride=72), :] for cp in range(2)], axis=1)
            new = old + add
            for cp in range(2):
                z_rows[cp, n, pl.ds(row, 32, stride=72), :] = new[:, cp * 128:cp * 128 + 128]
            s1 = s1 + jnp.sum(add.reshape(4, 8, 256), axis=0)
            s2 = s2 + jnp.sum((new * new - old * old).reshape(4, 8, 256), axis=0)
    send_sums(0, (s1, s2))
    for n in range(NB):
        for cp in range(2):
            hs[1, 0, n, cp * 32:cp * 32 + 32, :] = z_rows[cp, n, pl.ds(0, 32, stride=72), :]
    start, wait = exchange(1, False)
    start()

    for copy in w_copies[1:]:
        copy.wait()

    def down_tap(v, p):
        cols = []
        for jp in range(2):
            q = v - 2 * jp
            cols.append(wdv[p, q] if 0 <= q <= 2 else jnp.zeros((64, 128), BF16))
        return jnp.concatenate(cols, axis=1)

    for v in range(5):
        for rp in range(2):
            wdm[v * 128 + rp * 64:v * 128 + rp * 64 + 64, :] = down_tap(v, rp)
    for v in range(6):
        wdm[640 + v * 64:640 + v * 64 + 64, :] = down_tap(v, 2)

    def build_b(layer):
        for p in range(3):
            for u in range(4):
                for jp in range(2):
                    q = u - jp
                    blk = wbv[layer, p, q] if 0 <= q <= 2 else jnp.zeros((128, 128), BF16)
                    row = (p * 4 + u) * 128
                    wbm[layer, row:row + 128, jp * 128:jp * 128 + 128] = blk

    for k in (0, 2):
        sa1[k, 8, 0] = zero_tile
    for p in range(3):
        yb0[p, 0, 0] = zero_tile
        yb1[p, 8, 1] = zero_tile

    @pl.when(is_top)
    def _():
        zb[:, :, :, :, 7:8, :] = jnp.zeros((2, 2, NB, 16, 1, 128), F32)

    @pl.when(is_bottom)
    def _():
        hr[1, 1] = jnp.zeros(hr.shape[2:], F32)
        zb[:, :, :, :, 72:73, :] = jnp.zeros((2, 2, NB, 16, 1, 128), F32)

    gamma = jnp.concatenate([nav[0, 0:1, :]] * 2, axis=1)
    beta = jnp.concatenate([nav[0, 1:2, :]] * 2, axis=1)
    wait()
    for n in range(NB):
        for cp in range(2):
            z_rows[cp, n, pl.ds(64, 32, stride=72), :] = hr[1, 1, n, cp * 32:cp * 32 + 32, :]
    scale, shift = recv_sums(0, gamma, beta, float(NB * 128 * 64 * group), True)

    row_idx = lax.broadcasted_iota(jnp.int32, (64, 128), 0)
    lane_idx = lax.broadcasted_iota(jnp.int32, (64, 128), 1)
    low_lanes = lane_idx < 64
    cut_top = jnp.logical_and(row_idx == 0, is_top)
    cut_bottom = jnp.logical_and(row_idx == 63, is_bottom)

    def norm_a(n, half, dst):
        for j in range(17 - half):
            a = half * 16 + j
            for cp in range(2 if j < 16 else 1):
                y = jnp.maximum(za[cp, n, a, 0:64, :] * scale + shift, 0.0)
                dst[cp, j // 2, j % 2] = y.astype(BF16)
            z_next = jnp.where(low_lanes, za[0, n, a, 1:65, :], pltpu.roll(za[1, n, a, 1:65, :], 64, 1))
            y = jnp.maximum(z_next * scale + shift, 0.0)
            dst[2, j // 2, j % 2] = jnp.where(cut_bottom, 0.0, y).astype(BF16)

    def store_z(par, n, g0, z_val):
        for jp in range(2):
            zb[par, jp, n, g0:g0 + 8, 8:72, :] = z_val[:, jp * 128:jp * 128 + 128].reshape(8, 64, 128)

    def conv_down(n, half, src, carry):
        parts = [src[0, 0:8, 0], src[1, 0:8, 0], src[0, 0:8, 1], src[1, 0:8, 1], src[0, 1:9, 0],
                 src[2, 0:8, 0], src[2, 0:8, 1], src[2, 1:9, 0]]
        lhs = jnp.concatenate([x.reshape(512, 128) for x in parts], axis=1)
        z_val = jnp.dot(lhs, wdm[...], preferred_element_type=F32)
        store_z(0, n, half * 8, z_val)
        return sums(z_val, carry)

    norm_a(0, 0, sa0)

    def loop_down(n, carry):
        carry = conv_down(n, 0, sa0, carry)
        norm_a(n, 1, sa1)
        carry = conv_down(n, 1, sa1, carry)
        norm_a(lax.rem(n + 1, NB), 0, sa0)
        return carry

    pixels = float(NB * 64 * 32 * group)
    b_rows = zb.reshape(2, 2, NB, 16 * 80, 128)

    def finish(layer, par, carry, gamma, beta, halo):
        send_sums(layer, carry)
        if halo:
            for n in range(NB):
                for jp in range(2):
                    for side, row in ((0, 8), (1, 71)):
                        hs[layer + 1, side, n, jp * 16:jp * 16 + 16, :] = b_rows[par, jp, n, pl.ds(row, 16, stride=80), :]
            start, wait = exchange(layer + 1, True)
            start()
            build_b(layer - 1)
            wait()

            @pl.when(sp > 0)
            def _():
                for n in range(NB):
                    for jp in range(2):
                        b_rows[par, jp, n, pl.ds(7, 16, stride=80), :] = hr[layer + 1, 0, n, jp * 16:jp * 16 + 16, :]

            @pl.when(sp < sp_size - 1)
            def _():
                for n in range(NB):
                    for jp in range(2):
                        b_rows[par, jp, n, pl.ds(72, 16, stride=80), :] = hr[layer + 1, 1, n, jp * 16:jp * 16 + 16, :]
        return recv_sums(layer, gamma, beta, pixels, False)

    carry = lax.fori_loop(0, NB, loop_down, zero_sums)
    scale, shift = finish(1, 0, carry, ndv[0:1], ndv[1:2], True)

    for layer in range(3):
        par = layer % 2

        def norm_b(n, half, dst, par=par, scale=scale, shift=shift):
            for j in range(1 - half, 18 - half):
                col = half * 16 - 1 + j
                for p in range(3):
                    y = jnp.maximum(zb[par, col % 2, n, col // 2, 7 + p:71 + p, :] * scale + shift, 0.0)
                    if p == 0:
                        y = jnp.where(cut_top, 0.0, y)
                    if p == 2:
                        y = jnp.where(cut_bottom, 0.0, y)
                    dst[p, j // 2, j % 2] = y.astype(BF16)

        def conv_b(n, half, src, carry, layer=layer, par=par):
            parts = []
            for p in range(3):
                for u in range(4):
                    parts.append(src[p, u // 2:u // 2 + 8, u % 2].reshape(512, 128))
            z_val = jnp.dot(jnp.concatenate(parts, axis=1), wbm[layer], preferred_element_type=F32)
            store_z(1 - par, n, half * 8, z_val)
            return sums(z_val, carry)

        norm_b(0, 0, yb0)

        def loop_b(n, carry):
            carry = conv_b(n, 0, yb0, carry)
            norm_b(n, 1, yb1)
            carry = conv_b(n, 1, yb1, carry)
            norm_b(lax.rem(n + 1, NB), 0, yb0)
            return carry

        carry = lax.fori_loop(0, NB, loop_b, zero_sums)
        scale, shift = finish(layer + 2, 1 - par, carry, nbv[layer, 0:1], nbv[layer, 1:2], layer < 2)

    for n in range(NB):
        def norm_out(i, carry, n=n):
            for k in range(4):
                for jp in range(2):
                    g = i * 4 + k
                    y = jnp.maximum(zb[1, jp, n, g, 8:72, :] * scale + shift, 0.0)
                    o32[n, pl.ds(g * 2 + jp, 64, stride=33), :] = y
            return carry
        lax.fori_loop(0, 4, norm_out, 0)

        def pack_out(i, carry, n=n):
            for k in range(8):
                out[n, i * 8 + k] = o32[n, pl.ds((i * 8 + k) * 33, 32), :].astype(BF16)
            return carry
        lax.fori_loop(0, 8, pack_out, 0)


def solution(mesh):
    dp_size, sp_size = mesh.shape["dp"], mesh.shape["sp"]
    group = dp_size * sp_size

    def body(images, w_a, norm_a, w_down, norm_down, w_b, norm_b):
        img = jnp.transpose(images, (0, 2, 3, 1)).reshape(NB, 4096, 128)
        vm = pltpu.VMEM
        hbm_spec = pl.BlockSpec(memory_space=pltpu.HBM)
        return pl.pallas_call(
            functools.partial(fused_kernel, dp_size, sp_size),
            out_shape=jax.ShapeDtypeStruct((NB, 64, 32, 128), BF16),
            in_specs=[hbm_spec] * 7,
            out_specs=pl.BlockSpec(memory_space=pltpu.VMEM),
            scratch_shapes=[
                vm((NB, 4224, 128), BF16),
                vm((NB, 33, 144, 128), F32),
                vm((4, 9, 64, 128), BF16),
                vm((4, 9, 64, 128), BF16),
                vm((2, NB, 32, 72, 128), F32),
                vm((3, 9, 2, 64, 128), BF16),
                vm((3, 9, 2, 64, 128), BF16),
                vm((2, 2, NB, 16, 80, 128), F32),
                vm((3, 9, 2, 64, 128), BF16),
                vm((3, 9, 2, 64, 128), BF16),
                vm((1024, 256), BF16),
                vm((1024, 256), BF16),
                vm((3, 1536, 256), BF16),
                vm((1, 3, 3, 64, 64), BF16),
                vm((1, 2, 64), F32),
                vm((3, 3, 64, 128), BF16),
                vm((2, 128), F32),
                vm((3, 3, 3, 128, 128), BF16),
                vm((3, 2, 128), F32),
                vm((5, group, 2, 128), F32),
                vm((NB, 64 * 33, 128), F32),
                vm((5, 2, NB, 64, 128), F32),
                vm((5, 2, NB, 64, 128), F32),
                pltpu.SemaphoreType.DMA((NB,)),
                pltpu.SemaphoreType.DMA((6,)),
                pltpu.SemaphoreType.DMA((5,)),
                pltpu.SemaphoreType.DMA((5,)),
                pltpu.SemaphoreType.DMA((5, 2)),
                pltpu.SemaphoreType.DMA((5, 2)),
            ],
            compiler_params=pltpu.CompilerParams(
                collective_id=0, has_side_effects=True, vmem_limit_bytes=48 * 1024 * 1024),
        )(*[pltpu.with_memory_space_constraint(x, pltpu.HBM) for x in (img, w_a, norm_a, w_down, norm_down, w_b, norm_b)])

    act_spec = P(("pod", "dp"), "sp", None, None)
    return jax.shard_map(body, mesh=mesh, in_specs=(act_spec, P(), P(), P(), P(), P(), P()), out_specs=act_spec, check_vma=False)
```

```python
import functools

import jax
import jax.numpy as jnp
from jax import lax
from jax.experimental import pallas as pl
from jax.experimental.pallas import tpu as pltpu
from jax.sharding import PartitionSpec as P

EPS_VALUE = 1e-5
F32 = jnp.float32
BF16 = jnp.bfloat16
NB = 3
MESH = pl.DeviceIdType.MESH


def fused_kernel(dp_size, sp_size, img, wa, na, wd, nd, wb, nb, out,
                 xv, t32, pa0, pa1, za, sa0, sa1, zb, yb0, yb1, wam, wdm, wbm,
                 wav, nav, wdv, ndv, wbv, nbv, st, o32, hs, hr,
                 img_sem, w_sem, st_send, st_recv, halo_send, halo_recv):
    group = dp_size * sp_size
    pod = lax.axis_index("pod")
    dp = lax.axis_index("dp")
    sp = lax.axis_index("sp")
    me = dp * sp_size + sp
    is_top = sp == 0
    is_bottom = sp == sp_size - 1

    dp_order = [dp_size - 1 - dp, lax.rem(dp + 2, dp_size), dp + 1 - 2 * lax.rem(dp, 2), dp]
    sp_order = [lax.rem(sp + off, sp_size) for off in (2, 1, 3, 0)]
    peers = [(pod, d, s) for d in dp_order for s in sp_order][:group - 1]

    barrier = pltpu.get_barrier_semaphore()
    for peer in peers:
        pl.semaphore_signal(barrier, inc=1, device_id=peer, device_id_type=MESH)

    img_copies = [pltpu.make_async_copy(img.at[n], xv.at[n, pl.ds(64, 4096)], img_sem.at[n]) for n in range(NB)]
    w_copies = [pltpu.make_async_copy(src, dst, w_sem.at[i]) for i, (src, dst) in enumerate(
        [(wa, wav), (na, nav), (wd, wdv), (nd, ndv), (wb, wbv), (nb, nbv)])]
    for copy in (w_copies[0], *img_copies, *w_copies[1:]):
        copy.start()

    zero_tile = jnp.zeros((64, 128), BF16)
    zero_row = jnp.zeros((NB, 33, 1, 128), F32)
    for n in range(NB):
        xv[n, 0:64] = zero_tile
        xv[n, 4160:4224] = zero_tile
    t32[:, :, 7:8, :] = zero_row
    t32[:, :, 136:137, :] = zero_row

    w_copies[0].wait()
    zero64 = jnp.zeros((64, 64), BF16)
    for t in range(4):
        for u in range(4):
            parts = []
            for cp in range(2):
                for rp in range(2):
                    p, q = t - rp, u - cp
                    parts.append(wav[0, p, q] if 0 <= p <= 2 and 0 <= q <= 2 else zero64)
            row = t * 256 + u * 64
            wam[row:row + 64, :] = jnp.concatenate(parts, axis=1)

    for n in range(NB):
        img_copies[n].wait()

        def to_rows(i, carry, n=n):
            for j in range(11):
                a = i * 11 + j
                tile = xv[n, pl.ds(pl.multiple_of(a * 128, 128), 128), :]
                t32[n, a, 8:136, :] = tile.T.astype(F32)
            return carry
        lax.fori_loop(0, 3, to_rows, 0)

    def exchange(idx, has_down):
        up = pltpu.make_async_remote_copy(hs.at[idx, 0], hr.at[idx, 1], halo_send.at[idx, 0], halo_recv.at[idx, 0],
                                          device_id=(pod, dp, lax.rem(sp + sp_size - 1, sp_size)), device_id_type=MESH)
        down = None
        if has_down:
            down = pltpu.make_async_remote_copy(hs.at[idx, 1], hr.at[idx, 0], halo_send.at[idx, 1], halo_recv.at[idx, 1],
                                                device_id=(pod, dp, lax.rem(sp + 1, sp_size)), device_id_type=MESH)

        def start():
            @pl.when(sp > 0)
            def _():
                up.start()
            if has_down:
                @pl.when(sp < sp_size - 1)
                def _():
                    down.start()

        def wait():
            @pl.when(sp > 0)
            def _():
                up.wait_send()
                if has_down:
                    down.wait_recv()

            @pl.when(sp < sp_size - 1)
            def _():
                up.wait_recv()
                if has_down:
                    down.wait_send()
        return start, wait

    t_rows = t32.reshape(NB, 33 * 144, 128)
    for n in range(NB):
        hs[0, 0, n, 0:33, :] = t_rows[n, pl.ds(8, 33, stride=144), :]
        hs[0, 1, n, 0:33, :] = t_rows[n, pl.ds(135, 33, stride=144), :]
    pl.semaphore_wait(barrier, group - 1)
    start, wait_image = exchange(0, True)
    start()

    def split_rows(n, a0, dst):
        for j in range(9):
            for t in range(4):
                dst[t, j] = t32[n, a0 + j, pl.ds(7 + t, 64, stride=2), :].astype(BF16)

    def sums(z_val, carry):
        s1, s2 = carry
        z8 = z_val.reshape(-1, 8, 256)
        return s1 + jnp.sum(z8, axis=0), s2 + jnp.sum(z8 * z8, axis=0)

    zero_sums = (jnp.zeros((8, 256), F32), jnp.zeros((8, 256), F32))

    def send_sums(layer, carry):
        rows = []
        for s in carry:
            r = jnp.sum(s, axis=0, keepdims=True)
            rows.append(r[:, :128] + r[:, 128:])
        st[layer, me] = jnp.concatenate(rows, axis=0)
        for peer in peers:
            pltpu.make_async_remote_copy(st.at[layer, me], st.at[layer, me], st_send.at[layer], st_recv.at[layer],
                                         device_id=peer, device_id_type=MESH).start()

    def recv_sums(layer, gamma, beta, count, fold):
        others = st.at[layer, pl.ds(0, group - 1)]
        pltpu.make_async_copy(others, others, st_recv.at[layer]).wait()
        pltpu.make_async_copy(others, others, st_send.at[layer]).wait()
        total = jnp.sum(st[layer], axis=0)
        if fold:
            total = total + pltpu.roll(total, 64, 1)
        mean = total[0:1] / count
        var = total[1:2] / count - mean * mean
        scale = gamma * lax.rsqrt(var + EPS_VALUE)
        return scale, beta - mean * scale

    def conv_a(n, a0, src, carry):
        parts = []
        for t in range(4):
            parts.append(src[t, 0:8].reshape(512, 128))
            parts.append(src[t, 1:9].reshape(512, 128))
        z_val = jnp.dot(jnp.concatenate(parts, axis=1), wam[...], preferred_element_type=F32)
        for cp in range(2):
            za[cp, n, pl.ds(a0, 8), 0:64, :] = z_val[:, cp * 128:cp * 128 + 128].reshape(8, 64, 128)
        return sums(z_val, carry)

    split_rows(0, 0, pa0)

    def loop_a(i, carry):
        n, a0 = lax.div(i, 2), lax.rem(i, 2) * 16
        after = lax.rem(i + 1, 2 * NB)
        carry = conv_a(n, a0, pa0, carry)
        split_rows(n, a0 + 8, pa1)
        carry = conv_a(n, a0 + 8, pa1, carry)
        split_rows(lax.div(after, 2), lax.rem(after, 2) * 16, pa0)
        return carry

    carry = lax.fori_loop(0, 2 * NB, loop_a, zero_sums, unroll=True)

    wait_image()

    @pl.when(is_top)
    def _():
        hr[0, 0] = jnp.zeros(hr.shape[2:], F32)

    @pl.when(is_bottom)
    def _():
        hr[0, 1] = jnp.zeros(hr.shape[2:], F32)

    s1, s2 = carry
    z_rows = za.reshape(2, NB, 32 * 72, 128)
    for n in range(NB):
        for side, row, w_row in ((0, 0, 0), (1, 63, 768)):
            lhs = jnp.concatenate([hr[0, side, n, 0:32, :], hr[0, side, n, 1:33, :]], axis=1).astype(BF16)
            add = jnp.dot(lhs, wam[w_row:w_row + 256, :], preferred_element_type=F32)
            old = jnp.concatenate([z_rows[cp, n, pl.ds(row, 32, stride=72), :] for cp in range(2)], axis=1)
            new = old + add
            for cp in range(2):
                z_rows[cp, n, pl.ds(row, 32, stride=72), :] = new[:, cp * 128:cp * 128 + 128]
            s1 = s1 + jnp.sum(add.reshape(4, 8, 256), axis=0)
            s2 = s2 + jnp.sum((new * new - old * old).reshape(4, 8, 256), axis=0)
    send_sums(0, (s1, s2))
    for n in range(NB):
        for cp in range(2):
            hs[1, 0, n, cp * 32:cp * 32 + 32, :] = z_rows[cp, n, pl.ds(0, 32, stride=72), :]
    start, wait = exchange(1, False)
    start()

    for copy in w_copies[1:]:
        copy.wait()

    def down_tap(v, p):
        cols = []
        for jp in range(2):
            q = v - 2 * jp
            cols.append(wdv[p, q] if 0 <= q <= 2 else jnp.zeros((64, 128), BF16))
        return jnp.concatenate(cols, axis=1)

    for v in range(5):
        for rp in range(2):
            wdm[v * 128 + rp * 64:v * 128 + rp * 64 + 64, :] = down_tap(v, rp)
    for v in range(6):
        wdm[640 + v * 64:640 + v * 64 + 64, :] = down_tap(v, 2)

    def build_b(layer):
        for p in range(3):
            for u in range(4):
                for jp in range(2):
                    q = u - jp
                    blk = wbv[layer, p, q] if 0 <= q <= 2 else jnp.zeros((128, 128), BF16)
                    row = (p * 4 + u) * 128
                    wbm[layer, row:row + 128, jp * 128:jp * 128 + 128] = blk

    for k in (0, 2):
        sa1[k, 8, 0] = zero_tile
    for p in range(3):
        yb0[p, 0, 0] = zero_tile
        yb1[p, 8, 1] = zero_tile

    @pl.when(is_top)
    def _():
        zb[:, :, :, :, 7:8, :] = jnp.zeros((2, 2, NB, 16, 1, 128), F32)

    @pl.when(is_bottom)
    def _():
        hr[1, 1] = jnp.zeros(hr.shape[2:], F32)
        zb[:, :, :, :, 72:73, :] = jnp.zeros((2, 2, NB, 16, 1, 128), F32)

    gamma = jnp.concatenate([nav[0, 0:1, :]] * 2, axis=1)
    beta = jnp.concatenate([nav[0, 1:2, :]] * 2, axis=1)
    wait()
    for n in range(NB):
        for cp in range(2):
            z_rows[cp, n, pl.ds(64, 32, stride=72), :] = hr[1, 1, n, cp * 32:cp * 32 + 32, :]
    scale, shift = recv_sums(0, gamma, beta, float(NB * 128 * 64 * group), True)

    row_idx = lax.broadcasted_iota(jnp.int32, (64, 128), 0)
    lane_idx = lax.broadcasted_iota(jnp.int32, (64, 128), 1)
    low_lanes = lane_idx < 64
    cut_top = jnp.logical_and(row_idx == 0, is_top)
    cut_bottom = jnp.logical_and(row_idx == 63, is_bottom)

    def norm_a(n, half, dst):
        for j in range(17 - half):
            a = half * 16 + j
            for cp in range(2 if j < 16 else 1):
                y = jnp.maximum(za[cp, n, a, 0:64, :] * scale + shift, 0.0)
                dst[cp, j // 2, j % 2] = y.astype(BF16)
            z_next = jnp.where(low_lanes, za[0, n, a, 1:65, :], pltpu.roll(za[1, n, a, 1:65, :], 64, 1))
            y = jnp.maximum(z_next * scale + shift, 0.0)
            dst[2, j // 2, j % 2] = jnp.where(cut_bottom, 0.0, y).astype(BF16)

    def store_z(par, n, g0, z_val):
        for jp in range(2):
            zb[par, jp, n, g0:g0 + 8, 8:72, :] = z_val[:, jp * 128:jp * 128 + 128].reshape(8, 64, 128)

    def conv_down(n, half, src, carry):
        parts = [src[0, 0:8, 0], src[1, 0:8, 0], src[0, 0:8, 1], src[1, 0:8, 1], src[0, 1:9, 0],
                 src[2, 0:8, 0], src[2, 0:8, 1], src[2, 1:9, 0]]
        lhs = jnp.concatenate([x.reshape(512, 128) for x in parts], axis=1)
        z_val = jnp.dot(lhs, wdm[...], preferred_element_type=F32)
        store_z(0, n, half * 8, z_val)
        return sums(z_val, carry)

    norm_a(0, 0, sa0)

    def loop_down(n, carry):
        carry = conv_down(n, 0, sa0, carry)
        norm_a(n, 1, sa1)
        carry = conv_down(n, 1, sa1, carry)
        norm_a(lax.rem(n + 1, NB), 0, sa0)
        return carry

    pixels = float(NB * 64 * 32 * group)
    b_rows = zb.reshape(2, 2, NB, 16 * 80, 128)

    def finish(layer, par, carry, gamma, beta, halo):
        send_sums(layer, carry)
        if halo:
            for n in range(NB):
                for jp in range(2):
                    for side, row in ((0, 8), (1, 71)):
                        hs[layer + 1, side, n, jp * 16:jp * 16 + 16, :] = b_rows[par, jp, n, pl.ds(row, 16, stride=80), :]
            start, wait = exchange(layer + 1, True)
            start()
            build_b(layer - 1)
            wait()

            @pl.when(sp > 0)
            def _():
                for n in range(NB):
                    for jp in range(2):
                        b_rows[par, jp, n, pl.ds(7, 16, stride=80), :] = hr[layer + 1, 0, n, jp * 16:jp * 16 + 16, :]

            @pl.when(sp < sp_size - 1)
            def _():
                for n in range(NB):
                    for jp in range(2):
                        b_rows[par, jp, n, pl.ds(72, 16, stride=80), :] = hr[layer + 1, 1, n, jp * 16:jp * 16 + 16, :]
        return recv_sums(layer, gamma, beta, pixels, False)

    carry = lax.fori_loop(0, NB, loop_down, zero_sums, unroll=True)
    scale, shift = finish(1, 0, carry, ndv[0:1], ndv[1:2], True)

    for layer in range(3):
        par = layer % 2

        def norm_b(n, half, dst, par=par, scale=scale, shift=shift):
            for j in range(1 - half, 18 - half):
                col = half * 16 - 1 + j
                for p in range(3):
                    y = jnp.maximum(zb[par, col % 2, n, col // 2, 7 + p:71 + p, :] * scale + shift, 0.0)
                    if p == 0:
                        y = jnp.where(cut_top, 0.0, y)
                    if p == 2:
                        y = jnp.where(cut_bottom, 0.0, y)
                    dst[p, j // 2, j % 2] = y.astype(BF16)

        def conv_b(n, half, src, carry, layer=layer, par=par):
            parts = []
            for p in range(3):
                for u in range(4):
                    parts.append(src[p, u // 2:u // 2 + 8, u % 2].reshape(512, 128))
            z_val = jnp.dot(jnp.concatenate(parts, axis=1), wbm[layer], preferred_element_type=F32)
            store_z(1 - par, n, half * 8, z_val)
            return sums(z_val, carry)

        norm_b(0, 0, yb0)

        def loop_b(n, carry):
            carry = conv_b(n, 0, yb0, carry)
            norm_b(n, 1, yb1)
            carry = conv_b(n, 1, yb1, carry)
            norm_b(lax.rem(n + 1, NB), 0, yb0)
            return carry

        carry = lax.fori_loop(0, NB, loop_b, zero_sums, unroll=True)
        scale, shift = finish(layer + 2, 1 - par, carry, nbv[layer, 0:1], nbv[layer, 1:2], layer < 2)

    for n in range(NB):
        def norm_out(i, carry, n=n):
            for k in range(4):
                for jp in range(2):
                    g = i * 4 + k
                    y = jnp.maximum(zb[1, jp, n, g, 8:72, :] * scale + shift, 0.0)
                    o32[n, pl.ds(g * 2 + jp, 64, stride=33), :] = y
            return carry
        lax.fori_loop(0, 4, norm_out, 0)

        def pack_out(i, carry, n=n):
            for k in range(8):
                out[n, i * 8 + k] = o32[n, pl.ds((i * 8 + k) * 33, 32), :].astype(BF16)
            return carry
        lax.fori_loop(0, 8, pack_out, 0)


def solution(mesh):
    dp_size, sp_size = mesh.shape["dp"], mesh.shape["sp"]
    group = dp_size * sp_size

    def body(images, w_a, norm_a, w_down, norm_down, w_b, norm_b):
        img = jnp.transpose(images, (0, 2, 3, 1)).reshape(NB, 4096, 128)
        vm = pltpu.VMEM
        hbm_spec = pl.BlockSpec(memory_space=pltpu.HBM)
        return pl.pallas_call(
            functools.partial(fused_kernel, dp_size, sp_size),
            out_shape=jax.ShapeDtypeStruct((NB, 64, 32, 128), BF16),
            in_specs=[hbm_spec] * 7,
            out_specs=pl.BlockSpec(memory_space=pltpu.VMEM),
            scratch_shapes=[
                vm((NB, 4224, 128), BF16),
                vm((NB, 33, 144, 128), F32),
                vm((4, 9, 64, 128), BF16),
                vm((4, 9, 64, 128), BF16),
                vm((2, NB, 32, 72, 128), F32),
                vm((3, 9, 2, 64, 128), BF16),
                vm((3, 9, 2, 64, 128), BF16),
                vm((2, 2, NB, 16, 80, 128), F32),
                vm((3, 9, 2, 64, 128), BF16),
                vm((3, 9, 2, 64, 128), BF16),
                vm((1024, 256), BF16),
                vm((1024, 256), BF16),
                vm((3, 1536, 256), BF16),
                vm((1, 3, 3, 64, 64), BF16),
                vm((1, 2, 64), F32),
                vm((3, 3, 64, 128), BF16),
                vm((2, 128), F32),
                vm((3, 3, 3, 128, 128), BF16),
                vm((3, 2, 128), F32),
                vm((5, group, 2, 128), F32),
                vm((NB, 64 * 33, 128), F32),
                vm((5, 2, NB, 64, 128), F32),
                vm((5, 2, NB, 64, 128), F32),
                pltpu.SemaphoreType.DMA((NB,)),
                pltpu.SemaphoreType.DMA((6,)),
                pltpu.SemaphoreType.DMA((5,)),
                pltpu.SemaphoreType.DMA((5,)),
                pltpu.SemaphoreType.DMA((5, 2)),
                pltpu.SemaphoreType.DMA((5, 2)),
            ],
            compiler_params=pltpu.CompilerParams(
                collective_id=0, has_side_effects=True, vmem_limit_bytes=48 * 1024 * 1024),
        )(*[pltpu.with_memory_space_constraint(x, pltpu.HBM) for x in (img, w_a, norm_a, w_down, norm_down, w_b, norm_b)])

    act_spec = P(("pod", "dp"), "sp", None, None)
    return jax.shard_map(body, mesh=mesh, in_specs=(act_spec, P(), P(), P(), P(), P(), P()), out_specs=act_spec, check_vma=False)
```

```python
import functools

import jax
import jax.numpy as jnp
from jax import lax
from jax.experimental import pallas as pl
from jax.experimental.pallas import tpu as pltpu
from jax.sharding import PartitionSpec as P

EPS_VALUE = 1e-5
F32 = jnp.float32
BF16 = jnp.bfloat16
NB = 3
MESH = pl.DeviceIdType.MESH


def fused_kernel(dp_size, sp_size, img, wa, na, wd, nd, wb, nb, out,
                 xv, t32, pa0, pa1, za, sa0, sa1, zb, yb0, yb1, wam, wdm, wbm,
                 wav, nav, wdv, ndv, wbv, nbv, st, o32, hs, hr,
                 img_sem, w_sem, st_send, st_recv, halo_send, halo_recv):
    group = dp_size * sp_size
    pod = lax.axis_index("pod")
    dp = lax.axis_index("dp")
    sp = lax.axis_index("sp")
    me = dp * sp_size + sp
    is_top = sp == 0
    is_bottom = sp == sp_size - 1

    dp_order = [dp_size - 1 - dp, lax.rem(dp + 2, dp_size), dp + 1 - 2 * lax.rem(dp, 2), dp]
    sp_order = [lax.rem(sp + off, sp_size) for off in (2, 1, 3, 0)]
    peers = [(pod, d, s) for d in dp_order for s in sp_order][:group - 1]

    barrier = pltpu.get_barrier_semaphore()
    for peer in peers:
        pl.semaphore_signal(barrier, inc=1, device_id=peer, device_id_type=MESH)

    img_copies = [pltpu.make_async_copy(img.at[n], xv.at[n, pl.ds(64, 4096)], img_sem.at[n]) for n in range(NB)]
    w_copies = [pltpu.make_async_copy(src, dst, w_sem.at[i]) for i, (src, dst) in enumerate(
        [(wa, wav), (na, nav), (wd, wdv), (nd, ndv), (wb, wbv), (nb, nbv)])]
    for copy in (w_copies[0], *img_copies, *w_copies[1:]):
        copy.start()

    zero_tile = jnp.zeros((64, 128), BF16)
    zero_row = jnp.zeros((NB, 33, 1, 128), F32)
    for n in range(NB):
        xv[n, 0:64] = zero_tile
        xv[n, 4160:4224] = zero_tile
    t32[:, :, 7:8, :] = zero_row
    t32[:, :, 136:137, :] = zero_row

    w_copies[0].wait()
    zero64 = jnp.zeros((64, 64), BF16)
    for t in range(4):
        for u in range(4):
            parts = []
            for cp in range(2):
                for rp in range(2):
                    p, q = t - rp, u - cp
                    parts.append(wav[0, p, q] if 0 <= p <= 2 and 0 <= q <= 2 else zero64)
            row = t * 256 + u * 64
            wam[row:row + 64, :] = jnp.concatenate(parts, axis=1)

    def to_rows(n, first, last):
        for a in range(first, last):
            t32[n, a, 8:136, :] = xv[n, a * 128:a * 128 + 128, :].T.astype(F32)

    img_copies[0].wait()
    to_rows(0, 0, 33)

    def exchange(idx, has_down):
        up = pltpu.make_async_remote_copy(hs.at[idx, 0], hr.at[idx, 1], halo_send.at[idx, 0], halo_recv.at[idx, 0],
                                          device_id=(pod, dp, lax.rem(sp + sp_size - 1, sp_size)), device_id_type=MESH)
        down = None
        if has_down:
            down = pltpu.make_async_remote_copy(hs.at[idx, 1], hr.at[idx, 0], halo_send.at[idx, 1], halo_recv.at[idx, 1],
                                                device_id=(pod, dp, lax.rem(sp + 1, sp_size)), device_id_type=MESH)

        def start():
            @pl.when(sp > 0)
            def _():
                up.start()
            if has_down:
                @pl.when(sp < sp_size - 1)
                def _():
                    down.start()

        def wait():
            @pl.when(sp > 0)
            def _():
                up.wait_send()
                if has_down:
                    down.wait_recv()

            @pl.when(sp < sp_size - 1)
            def _():
                up.wait_recv()
                if has_down:
                    down.wait_send()
        return start, wait

    def split_rows(n, a0, dst):
        for j in range(9):
            for t in range(4):
                dst[t, j] = t32[n, a0 + j, pl.ds(7 + t, 64, stride=2), :].astype(BF16)

    def sums(z_val, carry):
        s1, s2 = carry
        z8 = z_val.reshape(-1, 8, 256)
        return s1 + jnp.sum(z8, axis=0), s2 + jnp.sum(z8 * z8, axis=0)

    zero_sums = (jnp.zeros((8, 256), F32), jnp.zeros((8, 256), F32))

    def send_sums(layer, carry):
        rows = []
        for s in carry:
            r = jnp.sum(s, axis=0, keepdims=True)
            rows.append(r[:, :128] + r[:, 128:])
        st[layer, me] = jnp.concatenate(rows, axis=0)
        for peer in peers:
            pltpu.make_async_remote_copy(st.at[layer, me], st.at[layer, me], st_send.at[layer], st_recv.at[layer],
                                         device_id=peer, device_id_type=MESH).start()

    def recv_sums(layer, gamma, beta, count, fold):
        others = st.at[layer, pl.ds(0, group - 1)]
        pltpu.make_async_copy(others, others, st_recv.at[layer]).wait()
        pltpu.make_async_copy(others, others, st_send.at[layer]).wait()
        total = jnp.sum(st[layer], axis=0)
        if fold:
            total = total + pltpu.roll(total, 64, 1)
        mean = total[0:1] / count
        var = total[1:2] / count - mean * mean
        scale = gamma * lax.rsqrt(var + EPS_VALUE)
        return scale, beta - mean * scale

    def conv_a(n, a0, src, carry):
        parts = []
        for t in range(4):
            parts.append(src[t, 0:8].reshape(512, 128))
            parts.append(src[t, 1:9].reshape(512, 128))
        z_val = jnp.dot(jnp.concatenate(parts, axis=1), wam[...], preferred_element_type=F32)
        for cp in range(2):
            za[cp, n, a0:a0 + 8, 0:64, :] = z_val[:, cp * 128:cp * 128 + 128].reshape(8, 64, 128)
        return sums(z_val, carry)

    split_rows(0, 0, pa0)
    img_copies[1].wait()
    t_rows = t32.reshape(NB, 33 * 144, 128)
    carry = zero_sums
    blocks = [(n, a0) for n in range(NB) for a0 in range(0, 32, 8)]
    for i, (n, a0) in enumerate(blocks):
        if i == 2:
            img_copies[2].wait()
        if i == 4:
            for k in range(NB):
                hs[0, 0, k, 0:33, :] = t_rows[k, pl.ds(8, 33, stride=144), :]
                hs[0, 1, k, 0:33, :] = t_rows[k, pl.ds(135, 33, stride=144), :]
            pl.semaphore_wait(barrier, group - 1)
            start, wait_image = exchange(0, True)
            start()
        carry = conv_a(n, a0, (pa0, pa1)[i % 2], carry)
        if i < 4:
            to_rows(1 + i // 2, (0, 17)[i % 2], (17, 33)[i % 2])
        if i + 1 < len(blocks):
            split_rows(*blocks[i + 1], (pa1, pa0)[i % 2])

    wait_image()

    @pl.when(is_top)
    def _():
        hr[0, 0] = jnp.zeros(hr.shape[2:], F32)

    @pl.when(is_bottom)
    def _():
        hr[0, 1] = jnp.zeros(hr.shape[2:], F32)

    s1, s2 = carry
    z_rows = za.reshape(2, NB, 32 * 72, 128)
    for n in range(NB):
        for side, row, w_row in ((0, 0, 0), (1, 63, 768)):
            lhs = jnp.concatenate([hr[0, side, n, 0:32, :], hr[0, side, n, 1:33, :]], axis=1).astype(BF16)
            add = jnp.dot(lhs, wam[w_row:w_row + 256, :], preferred_element_type=F32)
            old = jnp.concatenate([z_rows[cp, n, pl.ds(row, 32, stride=72), :] for cp in range(2)], axis=1)
            new = old + add
            for cp in range(2):
                z_rows[cp, n, pl.ds(row, 32, stride=72), :] = new[:, cp * 128:cp * 128 + 128]
            s1 = s1 + jnp.sum(add.reshape(4, 8, 256), axis=0)
            s2 = s2 + jnp.sum((new * new - old * old).reshape(4, 8, 256), axis=0)
    send_sums(0, (s1, s2))
    for n in range(NB):
        for cp in range(2):
            hs[1, 0, n, cp * 32:cp * 32 + 32, :] = z_rows[cp, n, pl.ds(0, 32, stride=72), :]
    start, wait = exchange(1, False)
    start()

    for copy in w_copies[1:]:
        copy.wait()

    def down_tap(v, p):
        cols = []
        for jp in range(2):
            q = v - 2 * jp
            cols.append(wdv[p, q] if 0 <= q <= 2 else jnp.zeros((64, 128), BF16))
        return jnp.concatenate(cols, axis=1)

    for v in range(5):
        for rp in range(2):
            wdm[v * 128 + rp * 64:v * 128 + rp * 64 + 64, :] = down_tap(v, rp)
    for v in range(6):
        wdm[640 + v * 64:640 + v * 64 + 64, :] = down_tap(v, 2)

    def build_b(layer):
        for p in range(3):
            for u in range(4):
                for jp in range(2):
                    q = u - jp
                    blk = wbv[layer, p, q] if 0 <= q <= 2 else jnp.zeros((128, 128), BF16)
                    row = (p * 4 + u) * 128
                    wbm[layer, row:row + 128, jp * 128:jp * 128 + 128] = blk

    for k in (0, 2):
        sa1[k, 8, 0] = zero_tile
    for p in range(3):
        yb0[p, 0, 0] = zero_tile
        yb1[p, 8, 1] = zero_tile

    @pl.when(is_top)
    def _():
        zb[:, :, :, :, 7:8, :] = jnp.zeros((2, 2, NB, 16, 1, 128), F32)

    @pl.when(is_bottom)
    def _():
        hr[1, 1] = jnp.zeros(hr.shape[2:], F32)
        zb[:, :, :, :, 72:73, :] = jnp.zeros((2, 2, NB, 16, 1, 128), F32)

    gamma = jnp.concatenate([nav[0, 0:1, :]] * 2, axis=1)
    beta = jnp.concatenate([nav[0, 1:2, :]] * 2, axis=1)
    wait()
    for n in range(NB):
        for cp in range(2):
            z_rows[cp, n, pl.ds(64, 32, stride=72), :] = hr[1, 1, n, cp * 32:cp * 32 + 32, :]
    scale, shift = recv_sums(0, gamma, beta, float(NB * 128 * 64 * group), True)

    row_idx = lax.broadcasted_iota(jnp.int32, (64, 128), 0)
    lane_idx = lax.broadcasted_iota(jnp.int32, (64, 128), 1)
    low_lanes = lane_idx < 64
    cut_top = jnp.logical_and(row_idx == 0, is_top)
    cut_bottom = jnp.logical_and(row_idx == 63, is_bottom)

    def norm_a(n, half, dst):
        for j in range(17 - half):
            a = half * 16 + j
            for cp in range(2 if j < 16 else 1):
                y = jnp.maximum(za[cp, n, a, 0:64, :] * scale + shift, 0.0)
                dst[cp, j // 2, j % 2] = y.astype(BF16)
            z_next = jnp.where(low_lanes, za[0, n, a, 1:65, :], pltpu.roll(za[1, n, a, 1:65, :], 64, 1))
            y = jnp.maximum(z_next * scale + shift, 0.0)
            dst[2, j // 2, j % 2] = jnp.where(cut_bottom, 0.0, y).astype(BF16)

    def store_z(par, n, g0, z_val):
        for jp in range(2):
            zb[par, jp, n, g0:g0 + 8, 8:72, :] = z_val[:, jp * 128:jp * 128 + 128].reshape(8, 64, 128)

    def conv_down(n, half, src, carry):
        parts = [src[0, 0:8, 0], src[1, 0:8, 0], src[0, 0:8, 1], src[1, 0:8, 1], src[0, 1:9, 0],
                 src[2, 0:8, 0], src[2, 0:8, 1], src[2, 1:9, 0]]
        lhs = jnp.concatenate([x.reshape(512, 128) for x in parts], axis=1)
        z_val = jnp.dot(lhs, wdm[...], preferred_element_type=F32)
        store_z(0, n, half * 8, z_val)
        return sums(z_val, carry)

    norm_a(0, 0, sa0)

    def loop_down(n, carry):
        carry = conv_down(n, 0, sa0, carry)
        norm_a(n, 1, sa1)
        carry = conv_down(n, 1, sa1, carry)
        norm_a(lax.rem(n + 1, NB), 0, sa0)
        return carry

    pixels = float(NB * 64 * 32 * group)
    b_rows = zb.reshape(2, 2, NB, 16 * 80, 128)

    def finish(layer, par, carry, gamma, beta, halo):
        send_sums(layer, carry)
        if halo:
            for n in range(NB):
                for jp in range(2):
                    for side, row in ((0, 8), (1, 71)):
                        hs[layer + 1, side, n, jp * 16:jp * 16 + 16, :] = b_rows[par, jp, n, pl.ds(row, 16, stride=80), :]
            start, wait = exchange(layer + 1, True)
            start()
            build_b(layer - 1)
            wait()

            @pl.when(sp > 0)
            def _():
                for n in range(NB):
                    for jp in range(2):
                        b_rows[par, jp, n, pl.ds(7, 16, stride=80), :] = hr[layer + 1, 0, n, jp * 16:jp * 16 + 16, :]

            @pl.when(sp < sp_size - 1)
            def _():
                for n in range(NB):
                    for jp in range(2):
                        b_rows[par, jp, n, pl.ds(72, 16, stride=80), :] = hr[layer + 1, 1, n, jp * 16:jp * 16 + 16, :]
        return recv_sums(layer, gamma, beta, pixels, False)

    carry = lax.fori_loop(0, NB, loop_down, zero_sums, unroll=True)
    scale, shift = finish(1, 0, carry, ndv[0:1], ndv[1:2], True)

    for layer in range(3):
        par = layer % 2

        def norm_b(n, half, dst, par=par, scale=scale, shift=shift):
            for j in range(1 - half, 18 - half):
                col = half * 16 - 1 + j
                for p in range(3):
                    y = jnp.maximum(zb[par, col % 2, n, col // 2, 7 + p:71 + p, :] * scale + shift, 0.0)
                    if p == 0:
                        y = jnp.where(cut_top, 0.0, y)
                    if p == 2:
                        y = jnp.where(cut_bottom, 0.0, y)
                    dst[p, j // 2, j % 2] = y.astype(BF16)

        def conv_b(n, half, src, carry, layer=layer, par=par):
            parts = []
            for p in range(3):
                for u in range(4):
                    parts.append(src[p, u // 2:u // 2 + 8, u % 2].reshape(512, 128))
            z_val = jnp.dot(jnp.concatenate(parts, axis=1), wbm[layer], preferred_element_type=F32)
            store_z(1 - par, n, half * 8, z_val)
            return sums(z_val, carry)

        norm_b(0, 0, yb0)

        def loop_b(n, carry):
            carry = conv_b(n, 0, yb0, carry)
            norm_b(n, 1, yb1)
            carry = conv_b(n, 1, yb1, carry)
            norm_b(lax.rem(n + 1, NB), 0, yb0)
            return carry

        carry = lax.fori_loop(0, NB, loop_b, zero_sums, unroll=True)
        scale, shift = finish(layer + 2, 1 - par, carry, nbv[layer, 0:1], nbv[layer, 1:2], layer < 2)

    for n in range(NB):
        def norm_out(i, carry, n=n):
            for k in range(4):
                for jp in range(2):
                    g = i * 4 + k
                    y = jnp.maximum(zb[1, jp, n, g, 8:72, :] * scale + shift, 0.0)
                    o32[n, pl.ds(g * 2 + jp, 64, stride=33), :] = y
            return carry
        lax.fori_loop(0, 4, norm_out, 0)

        def pack_out(i, carry, n=n):
            for k in range(8):
                out[n, i * 8 + k] = o32[n, pl.ds((i * 8 + k) * 33, 32), :].astype(BF16)
            return carry
        lax.fori_loop(0, 8, pack_out, 0)


def solution(mesh):
    dp_size, sp_size = mesh.shape["dp"], mesh.shape["sp"]
    group = dp_size * sp_size

    def body(images, w_a, norm_a, w_down, norm_down, w_b, norm_b):
        img = jnp.transpose(images, (0, 2, 3, 1)).reshape(NB, 4096, 128)
        vm = pltpu.VMEM
        hbm_spec = pl.BlockSpec(memory_space=pltpu.HBM)
        return pl.pallas_call(
            functools.partial(fused_kernel, dp_size, sp_size),
            out_shape=jax.ShapeDtypeStruct((NB, 64, 32, 128), BF16),
            in_specs=[hbm_spec] * 7,
            out_specs=pl.BlockSpec(memory_space=pltpu.VMEM),
            scratch_shapes=[
                vm((NB, 4224, 128), BF16),
                vm((NB, 33, 144, 128), F32),
                vm((4, 9, 64, 128), BF16),
                vm((4, 9, 64, 128), BF16),
                vm((2, NB, 32, 72, 128), F32),
                vm((3, 9, 2, 64, 128), BF16),
                vm((3, 9, 2, 64, 128), BF16),
                vm((2, 2, NB, 16, 80, 128), F32),
                vm((3, 9, 2, 64, 128), BF16),
                vm((3, 9, 2, 64, 128), BF16),
                vm((1024, 256), BF16),
                vm((1024, 256), BF16),
                vm((3, 1536, 256), BF16),
                vm((1, 3, 3, 64, 64), BF16),
                vm((1, 2, 64), F32),
                vm((3, 3, 64, 128), BF16),
                vm((2, 128), F32),
                vm((3, 3, 3, 128, 128), BF16),
                vm((3, 2, 128), F32),
                vm((5, group, 2, 128), F32),
                vm((NB, 64 * 33, 128), F32),
                vm((5, 2, NB, 64, 128), F32),
                vm((5, 2, NB, 64, 128), F32),
                pltpu.SemaphoreType.DMA((NB,)),
                pltpu.SemaphoreType.DMA((6,)),
                pltpu.SemaphoreType.DMA((5,)),
                pltpu.SemaphoreType.DMA((5,)),
                pltpu.SemaphoreType.DMA((5, 2)),
                pltpu.SemaphoreType.DMA((5, 2)),
            ],
            compiler_params=pltpu.CompilerParams(
                collective_id=0, has_side_effects=True, vmem_limit_bytes=48 * 1024 * 1024),
        )(*[pltpu.with_memory_space_constraint(x, pltpu.HBM) for x in (img, w_a, norm_a, w_down, norm_down, w_b, norm_b)])

    act_spec = P(("pod", "dp"), "sp", None, None)
    return jax.shard_map(body, mesh=mesh, in_specs=(act_spec, P(), P(), P(), P(), P(), P()), out_specs=act_spec, check_vma=False)
```

```python
import functools

import jax
import jax.numpy as jnp
from jax import lax
from jax.experimental import pallas as pl
from jax.experimental.pallas import tpu as pltpu
from jax.sharding import PartitionSpec as P

EPS_VALUE = 1e-5
F32 = jnp.float32
BF16 = jnp.bfloat16
NB = 3
MESH = pl.DeviceIdType.MESH


def fused_kernel(dp_size, sp_size, img, wa, na, wd, nd, wb, nb, out,
                 xv, t32, pa0, pa1, za, sa0, sa1, zb, yb0, yb1, wam, wdm, wbm,
                 wav, nav, wdv, ndv, wbv, nbv, st, o32, hs, hr,
                 img_sem, w_sem, st_send, st_recv, halo_send, halo_recv):
    group = dp_size * sp_size
    pod = lax.axis_index("pod")
    dp = lax.axis_index("dp")
    sp = lax.axis_index("sp")
    me = dp * sp_size + sp
    is_top = sp == 0
    is_bottom = sp == sp_size - 1

    dp_order = [dp_size - 1 - dp, lax.rem(dp + 2, dp_size), dp + 1 - 2 * lax.rem(dp, 2), dp]
    sp_order = [lax.rem(sp + off, sp_size) for off in (2, 1, 3, 0)]
    peers = [(pod, d, s) for d in dp_order for s in sp_order][:group - 1]

    barrier = pltpu.get_barrier_semaphore()
    for peer in peers:
        pl.semaphore_signal(barrier, inc=1, device_id=peer, device_id_type=MESH)

    img_copies = [pltpu.make_async_copy(img.at[n], xv.at[n, pl.ds(64, 4096)], img_sem.at[n]) for n in range(NB)]
    w_copies = [pltpu.make_async_copy(src, dst, w_sem.at[i]) for i, (src, dst) in enumerate(
        [(wa, wav), (na, nav), (wd, wdv), (nd, ndv), (wb, wbv), (nb, nbv)])]
    for copy in (w_copies[0], *img_copies, *w_copies[1:]):
        copy.start()

    zero_tile = jnp.zeros((64, 128), BF16)
    zero_row = jnp.zeros((NB, 33, 1, 128), F32)
    for n in range(NB):
        xv[n, 0:64] = zero_tile
        xv[n, 4160:4224] = zero_tile
    t32[:, :, 7:8, :] = zero_row
    t32[:, :, 136:137, :] = zero_row

    w_copies[0].wait()
    zero64 = jnp.zeros((64, 64), BF16)
    for t in range(4):
        for u in range(4):
            parts = []
            for cp in range(2):
                for rp in range(2):
                    p, q = t - rp, u - cp
                    parts.append(wav[0, p, q] if 0 <= p <= 2 and 0 <= q <= 2 else zero64)
            row = t * 256 + u * 64
            wam[row:row + 64, :] = jnp.concatenate(parts, axis=1)

    def to_rows(n, first, last):
        for a in range(first, last):
            t32[n, a, 8:136, :] = xv[n, a * 128:a * 128 + 128, :].T.astype(F32)

    img_copies[0].wait()
    to_rows(0, 0, 33)

    def exchange(idx, has_down):
        up = pltpu.make_async_remote_copy(hs.at[idx, 0], hr.at[idx, 1], halo_send.at[idx, 0], halo_recv.at[idx, 0],
                                          device_id=(pod, dp, lax.rem(sp + sp_size - 1, sp_size)), device_id_type=MESH)
        down = None
        if has_down:
            down = pltpu.make_async_remote_copy(hs.at[idx, 1], hr.at[idx, 0], halo_send.at[idx, 1], halo_recv.at[idx, 1],
                                                device_id=(pod, dp, lax.rem(sp + 1, sp_size)), device_id_type=MESH)

        def start():
            @pl.when(sp > 0)
            def _():
                up.start()
            if has_down:
                @pl.when(sp < sp_size - 1)
                def _():
                    down.start()

        def wait():
            @pl.when(sp > 0)
            def _():
                up.wait_send()
                if has_down:
                    down.wait_recv()

            @pl.when(sp < sp_size - 1)
            def _():
                up.wait_recv()
                if has_down:
                    down.wait_send()
        return start, wait

    def split_rows(n, a0, dst):
        for j in range(9):
            for t in range(4):
                dst[t, j] = t32[n, a0 + j, pl.ds(7 + t, 64, stride=2), :].astype(BF16)

    def sums(z_val, carry):
        s1, s2 = carry
        z8 = z_val.reshape(-1, 8, 256)
        return s1 + jnp.sum(z8, axis=0), s2 + jnp.sum(z8 * z8, axis=0)

    zero_sums = (jnp.zeros((8, 256), F32), jnp.zeros((8, 256), F32))

    def send_sums(layer, carry):
        rows = []
        for s in carry:
            r = jnp.sum(s, axis=0, keepdims=True)
            rows.append(r[:, :128] + r[:, 128:])
        st[layer, me] = jnp.concatenate(rows, axis=0)
        for peer in peers:
            pltpu.make_async_remote_copy(st.at[layer, me], st.at[layer, me], st_send.at[layer], st_recv.at[layer],
                                         device_id=peer, device_id_type=MESH).start()

    def recv_sums(layer, gamma, beta, count, fold):
        others = st.at[layer, pl.ds(0, group - 1)]
        pltpu.make_async_copy(others, others, st_recv.at[layer]).wait()
        pltpu.make_async_copy(others, others, st_send.at[layer]).wait()
        total = jnp.sum(st[layer], axis=0)
        if fold:
            total = total + pltpu.roll(total, 64, 1)
        mean = total[0:1] / count
        var = total[1:2] / count - mean * mean
        scale = gamma * lax.rsqrt(var + EPS_VALUE)
        return scale, beta - mean * scale

    def conv_a(n, a0, src, carry):
        parts = []
        for t in range(4):
            parts.append(src[t, 0:8].reshape(512, 128))
            parts.append(src[t, 1:9].reshape(512, 128))
        z_val = jnp.dot(jnp.concatenate(parts, axis=1), wam[...], preferred_element_type=F32)
        for cp in range(2):
            za[cp, n, a0:a0 + 8, 0:64, :] = z_val[:, cp * 128:cp * 128 + 128].reshape(8, 64, 128)
        return sums(z_val, carry)

    split_rows(0, 0, pa0)
    img_copies[1].wait()
    t_rows = t32.reshape(NB, 33 * 144, 128)
    carry = zero_sums
    blocks = [(n, a0) for n in range(NB) for a0 in range(0, 32, 8)]
    for i, (n, a0) in enumerate(blocks):
        if i == 2:
            img_copies[2].wait()
        if i == 4:
            for k in range(NB):
                hs[0, 0, k, 0:33, :] = t_rows[k, pl.ds(8, 33, stride=144), :]
                hs[0, 1, k, 0:33, :] = t_rows[k, pl.ds(135, 33, stride=144), :]
            pl.semaphore_wait(barrier, group - 1)
            start, wait_image = exchange(0, True)
            start()
        carry = conv_a(n, a0, (pa0, pa1)[i % 2], carry)
        if i < 4:
            to_rows(1 + i // 2, (0, 17)[i % 2], (17, 33)[i % 2])
        if i + 1 < len(blocks):
            split_rows(*blocks[i + 1], (pa1, pa0)[i % 2])

    wait_image()

    @pl.when(is_top)
    def _():
        hr[0, 0] = jnp.zeros(hr.shape[2:], F32)

    @pl.when(is_bottom)
    def _():
        hr[0, 1] = jnp.zeros(hr.shape[2:], F32)

    s1, s2 = carry
    z_rows = za.reshape(2, NB, 32 * 72, 128)
    for n in range(NB):
        for side, row, w_row in ((0, 0, 0), (1, 63, 768)):
            lhs = jnp.concatenate([hr[0, side, n, 0:32, :], hr[0, side, n, 1:33, :]], axis=1).astype(BF16)
            add = jnp.dot(lhs, wam[w_row:w_row + 256, :], preferred_element_type=F32)
            old = jnp.concatenate([z_rows[cp, n, pl.ds(row, 32, stride=72), :] for cp in range(2)], axis=1)
            new = old + add
            for cp in range(2):
                z_rows[cp, n, pl.ds(row, 32, stride=72), :] = new[:, cp * 128:cp * 128 + 128]
            s1 = s1 + jnp.sum(add.reshape(4, 8, 256), axis=0)
            s2 = s2 + jnp.sum((new * new - old * old).reshape(4, 8, 256), axis=0)
    send_sums(0, (s1, s2))
    for n in range(NB):
        for cp in range(2):
            hs[1, 0, n, cp * 32:cp * 32 + 32, :] = z_rows[cp, n, pl.ds(0, 32, stride=72), :]
    start, wait = exchange(1, False)
    start()

    for copy in w_copies[1:]:
        copy.wait()

    def down_tap(v, p):
        cols = []
        for jp in range(2):
            q = v - 2 * jp
            cols.append(wdv[p, q] if 0 <= q <= 2 else jnp.zeros((64, 128), BF16))
        return jnp.concatenate(cols, axis=1)

    for v in range(5):
        for rp in range(2):
            wdm[v * 128 + rp * 64:v * 128 + rp * 64 + 64, :] = down_tap(v, rp)
    for v in range(6):
        wdm[640 + v * 64:640 + v * 64 + 64, :] = down_tap(v, 2)

    def build_b(layer):
        for p in range(3):
            for u in range(4):
                for jp in range(2):
                    q = u - jp
                    blk = wbv[layer, p, q] if 0 <= q <= 2 else jnp.zeros((128, 128), BF16)
                    row = (p * 4 + u) * 128
                    wbm[layer, row:row + 128, jp * 128:jp * 128 + 128] = blk

    for k in (0, 2):
        sa1[k, 8, 0] = zero_tile
    for p in range(3):
        yb0[p, 0, 0] = zero_tile
        yb1[p, 8, 1] = zero_tile

    @pl.when(is_top)
    def _():
        zb[:, :, :, :, 7:8, :] = jnp.zeros((2, 2, NB, 16, 1, 128), F32)

    @pl.when(is_bottom)
    def _():
        hr[1, 1] = jnp.zeros(hr.shape[2:], F32)
        zb[:, :, :, :, 72:73, :] = jnp.zeros((2, 2, NB, 16, 1, 128), F32)

    gamma = jnp.concatenate([nav[0, 0:1, :]] * 2, axis=1)
    beta = jnp.concatenate([nav[0, 1:2, :]] * 2, axis=1)
    wait()
    for n in range(NB):
        for cp in range(2):
            z_rows[cp, n, pl.ds(64, 32, stride=72), :] = hr[1, 1, n, cp * 32:cp * 32 + 32, :]
    scale, shift = recv_sums(0, gamma, beta, float(NB * 128 * 64 * group), True)

    row_idx = lax.broadcasted_iota(jnp.int32, (64, 128), 0)
    lane_idx = lax.broadcasted_iota(jnp.int32, (64, 128), 1)
    low_lanes = lane_idx < 64
    cut_top = jnp.logical_and(row_idx == 0, is_top)
    cut_bottom = jnp.logical_and(row_idx == 63, is_bottom)

    def norm_a(n, half, dst):
        for j in range(17 - half):
            a = half * 16 + j
            for cp in range(2 if j < 16 else 1):
                y = jnp.maximum(za[cp, n, a, 0:64, :] * scale + shift, 0.0)
                dst[cp, j // 2, j % 2] = y.astype(BF16)
            z_next = jnp.where(low_lanes, za[0, n, a, 1:65, :], pltpu.roll(za[1, n, a, 1:65, :], 64, 1))
            y = jnp.maximum(z_next * scale + shift, 0.0)
            dst[2, j // 2, j % 2] = jnp.where(cut_bottom, 0.0, y).astype(BF16)

    def store_z(par, n, g0, z_val):
        for jp in range(2):
            zb[par, jp, n, g0:g0 + 8, 8:72, :] = z_val[:, jp * 128:jp * 128 + 128].reshape(8, 64, 128)

    def conv_down(n, half, src, carry):
        parts = [src[0, 0:8, 0], src[1, 0:8, 0], src[0, 0:8, 1], src[1, 0:8, 1], src[0, 1:9, 0],
                 src[2, 0:8, 0], src[2, 0:8, 1], src[2, 1:9, 0]]
        lhs = jnp.concatenate([x.reshape(512, 128) for x in parts], axis=1)
        z_val = jnp.dot(lhs, wdm[...], preferred_element_type=F32)
        store_z(0, n, half * 8, z_val)
        return sums(z_val, carry)

    norm_a(0, 0, sa0)

    def loop_down(n, carry):
        carry = conv_down(n, 0, sa0, carry)
        norm_a(n, 1, sa1)
        carry = conv_down(n, 1, sa1, carry)
        if n + 1 < NB:
            norm_a(n + 1, 0, sa0)
        return carry

    pixels = float(NB * 64 * 32 * group)
    b_rows = zb.reshape(2, 2, NB, 16 * 80, 128)

    def finish(layer, par, carry, gamma, beta, halo):
        send_sums(layer, carry)
        if halo:
            for n in range(NB):
                for jp in range(2):
                    for side, row in ((0, 8), (1, 71)):
                        hs[layer + 1, side, n, jp * 16:jp * 16 + 16, :] = b_rows[par, jp, n, pl.ds(row, 16, stride=80), :]
            start, wait = exchange(layer + 1, True)
            start()
            build_b(layer - 1)
            wait()

            @pl.when(sp > 0)
            def _():
                for n in range(NB):
                    for jp in range(2):
                        b_rows[par, jp, n, pl.ds(7, 16, stride=80), :] = hr[layer + 1, 0, n, jp * 16:jp * 16 + 16, :]

            @pl.when(sp < sp_size - 1)
            def _():
                for n in range(NB):
                    for jp in range(2):
                        b_rows[par, jp, n, pl.ds(72, 16, stride=80), :] = hr[layer + 1, 1, n, jp * 16:jp * 16 + 16, :]
        return recv_sums(layer, gamma, beta, pixels, False)

    carry = zero_sums
    for n in range(NB):
        carry = loop_down(n, carry)
    scale, shift = finish(1, 0, carry, ndv[0:1], ndv[1:2], True)

    for layer in range(3):
        par = layer % 2

        def norm_b(n, half, dst, par=par, scale=scale, shift=shift):
            for j in range(1 - half, 18 - half):
                col = half * 16 - 1 + j
                for p in range(3):
                    y = jnp.maximum(zb[par, col % 2, n, col // 2, 7 + p:71 + p, :] * scale + shift, 0.0)
                    if p == 0:
                        y = jnp.where(cut_top, 0.0, y)
                    if p == 2:
                        y = jnp.where(cut_bottom, 0.0, y)
                    dst[p, j // 2, j % 2] = y.astype(BF16)

        def conv_b(n, half, src, carry, layer=layer, par=par):
            parts = []
            for p in range(3):
                for u in range(4):
                    parts.append(src[p, u // 2:u // 2 + 8, u % 2].reshape(512, 128))
            z_val = jnp.dot(jnp.concatenate(parts, axis=1), wbm[layer], preferred_element_type=F32)
            store_z(1 - par, n, half * 8, z_val)
            return sums(z_val, carry)

        norm_b(0, 0, yb0)

        def loop_b(n, carry):
            carry = conv_b(n, 0, yb0, carry)
            norm_b(n, 1, yb1)
            carry = conv_b(n, 1, yb1, carry)
            if n + 1 < NB:
                norm_b(n + 1, 0, yb0)
            return carry

        carry = zero_sums
        for n in range(NB):
            carry = loop_b(n, carry)
        scale, shift = finish(layer + 2, 1 - par, carry, nbv[layer, 0:1], nbv[layer, 1:2], layer < 2)

    for n in range(NB):
        def norm_out(i, carry, n=n):
            for k in range(4):
                for jp in range(2):
                    g = i * 4 + k
                    y = jnp.maximum(zb[1, jp, n, g, 8:72, :] * scale + shift, 0.0)
                    o32[n, pl.ds(g * 2 + jp, 64, stride=33), :] = y
            return carry
        lax.fori_loop(0, 4, norm_out, 0)

        def pack_out(i, carry, n=n):
            for k in range(8):
                out[n, i * 8 + k] = o32[n, pl.ds((i * 8 + k) * 33, 32), :].astype(BF16)
            return carry
        lax.fori_loop(0, 8, pack_out, 0)


def solution(mesh):
    dp_size, sp_size = mesh.shape["dp"], mesh.shape["sp"]
    group = dp_size * sp_size

    def body(images, w_a, norm_a, w_down, norm_down, w_b, norm_b):
        img = jnp.transpose(images, (0, 2, 3, 1)).reshape(NB, 4096, 128)
        vm = pltpu.VMEM
        hbm_spec = pl.BlockSpec(memory_space=pltpu.HBM)
        return pl.pallas_call(
            functools.partial(fused_kernel, dp_size, sp_size),
            out_shape=jax.ShapeDtypeStruct((NB, 64, 32, 128), BF16),
            in_specs=[hbm_spec] * 7,
            out_specs=pl.BlockSpec(memory_space=pltpu.VMEM),
            scratch_shapes=[
                vm((NB, 4224, 128), BF16),
                vm((NB, 33, 144, 128), F32),
                vm((4, 9, 64, 128), BF16),
                vm((4, 9, 64, 128), BF16),
                vm((2, NB, 32, 72, 128), F32),
                vm((3, 9, 2, 64, 128), BF16),
                vm((3, 9, 2, 64, 128), BF16),
                vm((2, 2, NB, 16, 80, 128), F32),
                vm((3, 9, 2, 64, 128), BF16),
                vm((3, 9, 2, 64, 128), BF16),
                vm((1024, 256), BF16),
                vm((1024, 256), BF16),
                vm((3, 1536, 256), BF16),
                vm((1, 3, 3, 64, 64), BF16),
                vm((1, 2, 64), F32),
                vm((3, 3, 64, 128), BF16),
                vm((2, 128), F32),
                vm((3, 3, 3, 128, 128), BF16),
                vm((3, 2, 128), F32),
                vm((5, group, 2, 128), F32),
                vm((NB, 64 * 33, 128), F32),
                vm((5, 2, NB, 64, 128), F32),
                vm((5, 2, NB, 64, 128), F32),
                pltpu.SemaphoreType.DMA((NB,)),
                pltpu.SemaphoreType.DMA((6,)),
                pltpu.SemaphoreType.DMA((5,)),
                pltpu.SemaphoreType.DMA((5,)),
                pltpu.SemaphoreType.DMA((5, 2)),
                pltpu.SemaphoreType.DMA((5, 2)),
            ],
            compiler_params=pltpu.CompilerParams(
                collective_id=0, has_side_effects=True, vmem_limit_bytes=48 * 1024 * 1024),
        )(*[pltpu.with_memory_space_constraint(x, pltpu.HBM) for x in (img, w_a, norm_a, w_down, norm_down, w_b, norm_b)])

    act_spec = P(("pod", "dp"), "sp", None, None)
    return jax.shard_map(body, mesh=mesh, in_specs=(act_spec, P(), P(), P(), P(), P(), P()), out_specs=act_spec, check_vma=False)
```
